32 devices in a mesh: groups: 2 (over x), tm: 8 (over z, y), tile: 2 (over core).
Axes of the slice: x: 2, y: 2, z: 4, core: 2. Of those that a mesh axis runs over, the one named last changes fastest.
Arguments:
- movie: bfloat16 [4, 2304, 4096], P(('groups', 'tile'), None, 'tm'), parts along dimension 0, may hold values from 0 to 4
- cycle_weights: bfloat16 [4, 2304, 56], P(('groups', 'tile')), parts along dimension 0, may hold values from -0.75 to 0.75
- footprints: bfloat16 [4, 2304, 384], P(('groups', 'tile')), parts along dimension 0, may hold values from 0.19921875 to 1
- traces: bfloat16 [4, 384, 4096], P(('groups', 'tile'), None, 'tm'), parts along dimension 0, may hold values from 0 to 1.5
- centre_row: int32 [4, 384], P(('groups', 'tile')), parts along dimension 0, may hold values from 0 to 47
- centre_col: int32 [4, 384], P(('groups', 'tile')), parts along dimension 0, may hold values from 0 to 47
- radius: int32 [4, 384], P(('groups', 'tile')), parts along dimension 0, may hold values from 4 to 9
- comp_count: int32 [4], P(('groups', 'tile')), parts along dimension 0, may hold values from 64 to 384
Outputs:
- new_footprints: bfloat16 [4, 2304, 384], P(('groups', 'tile')), parts along dimension 0
- new_traces: bfloat16 [4, 384, 4096], P(('groups', 'tile'), None, 'tm'), parts along dimension 0
The draws below stay inside these ranges and needn't reach their ends.
There are 2 independent parts, one for each index of `groups`. The reference program is written for one: setup_inputs(seed, part) draws one part's arguments, and reference() takes and returns one part's arrays. A program takes and returns all parts, laid end to end along the dimension named above; each array names one. Nothing has to cross between parts.
All inputs are finite; a program needn't handle non-finite values.
Results may differ from the reference program's by a relative error of at most 0.0034.
Values may be sent and summed in bfloat16 or wider, within the bound.
A program may use at most 64 MiB of HBM per device.

```python
import math
import jax
import jax.numpy as jnp
from jax import lax

TILE_SIDE = 48
CYCLE = 8
OFFS = 56
KMAX = 384
PASSES = 2
PIX = 2304
TILES = 2
FRAMES = 4096


def draw_traces(key, part):
    first_key = jax.random.fold_in(jax.random.fold_in(key, 17), 0)
    ramp = 1.0 + 2.0 * jnp.arange(FRAMES, dtype=jnp.float32) / FRAMES
    logs = jax.random.uniform(first_key, (TILES, KMAX, FRAMES), jnp.float32, math.log(0.05), math.log(0.5))
    values = jnp.exp(logs) * ramp[None, None, :]
    return values.astype(jnp.bfloat16)


def place_ends(entries, stream_key, low, largest):
    dims = entries.shape
    index_at = [jax.random.randint(jax.random.fold_in(stream_key, axis), (), 0, dims[axis]) for axis in range(len(dims))]
    entries = entries.at[tuple(index_at)].set(low)
    longest = dims.index(max(dims))
    index_at[longest] = (index_at[longest] + 1) % dims[longest]
    return entries.at[tuple(index_at)].set(largest)


def steps_of(key, extent, shards, least, largest):
    gain, own = 1.0, jax.random.fold_in(key, 6)
    for position, blocks in shards:
        steps = jnp.exp(jax.random.uniform(jax.random.fold_in(own, position), (blocks,), jnp.float32, least / len(shards), largest / len(shards)))
        gain = gain * jnp.repeat(steps, extent[position] // blocks).reshape([-1 if axis == position else 1 for axis in range(len(extent))])
    return gain


def bell_draw(own_key, dims, spread, bound, pieces=(), held_as=jnp.bfloat16):
    array = jax.random.normal(own_key, dims, jnp.float32) * spread
    if len(pieces) > 0:
        array = steps_of(own_key, dims, pieces, -0.22, 0.18) * array
    return jnp.clip(array, min=-bound, max=bound).astype(held_as)


def setup_inputs(seed: int = 0, part: int = 0) -> dict:
    splits = jax.random.split(jax.random.key(seed), 9)
    own_keys = jax.random.split(jax.random.fold_in(splits[8], part), 9)
    return {
        "movie": jnp.clip(4.0 * jax.random.uniform(own_keys[0], (TILES, PIX, FRAMES), jnp.float32) ** steps_of(own_keys[0], (TILES, PIX, FRAMES), ((0, 2), (2, 8)), -0.2, 0.2), 0.0, 4.0).astype(jnp.bfloat16),
        "cycle_weights": bell_draw(own_keys[1], (TILES, PIX, OFFS), OFFS ** -0.5, 0.75, ((0, 2),)),
        "footprints": jnp.clip(0.19921875 + 0.80078125 * jax.random.uniform(own_keys[2], (TILES, PIX, KMAX), jnp.float32) ** steps_of(own_keys[2], (TILES, PIX, KMAX), ((0, 2),), -0.2, 0.2), 0.19921875, 1.0).astype(jnp.bfloat16),
        "traces": draw_traces(jax.random.fold_in(jax.random.fold_in(splits[8], part), 71), part),
        "centre_row": place_ends(jax.random.randint(own_keys[4], (TILES, KMAX), 0, TILE_SIDE), jax.random.fold_in(own_keys[4], 1), 0, TILE_SIDE - 1).astype(jnp.int32),
        "centre_col": place_ends(jax.random.randint(own_keys[5], (TILES, KMAX), 0, TILE_SIDE), jax.random.fold_in(own_keys[5], 1), 0, TILE_SIDE - 1).astype(jnp.int32),
        "radius": place_ends(jax.random.randint(own_keys[6], (TILES, KMAX), TILE_SIDE // 12, TILE_SIDE // 5 + 1), jax.random.fold_in(own_keys[6], 1), TILE_SIDE // 12, (TILE_SIDE // 5 + 1) - 1).astype(jnp.int32),
        "comp_count": jax.random.randint(own_keys[7], (TILES,), KMAX // 6, KMAX + 1).astype(jnp.int32),
    }


RIDGE_TERM = 1.0


def cycle_offsets():
    found = []
    for row_step in range(-CYCLE, CYCLE + 1):
        for col_step in range(-CYCLE, CYCLE + 1):
            dist_sq = row_step * row_step + col_step * col_step
            if CYCLE * CYCLE <= dist_sq < (CYCLE + 1) * (CYCLE + 1):
                found.append((row_step, col_step))
    return found


def cycle_back(weights, window):
    frames = window.shape[2]
    grid_w = weights.reshape(TILE_SIDE, TILE_SIDE, -1)
    total = jnp.zeros((TILE_SIDE, TILE_SIDE, frames), jnp.float32)
    for index, (row_step, col_step) in enumerate(cycle_offsets()):
        top = CYCLE + row_step
        left = CYCLE + col_step
        piece = window[top:top + TILE_SIDE, left:left + TILE_SIDE, :].astype(jnp.float32)
        total = total + grid_w[:, :, index:index + 1].astype(jnp.float32) * piece
    return total.reshape(TILE_SIDE * TILE_SIDE, frames).astype(jnp.bfloat16)


def keep_mask(row_at, col_at, reach, count):
    pixel = jnp.arange(TILE_SIDE * TILE_SIDE, dtype=jnp.int32)
    row_gap = (pixel // TILE_SIDE)[:, None] - row_at[None, :]
    col_gap = (pixel % TILE_SIDE)[:, None] - col_at[None, :]
    inside = row_gap * row_gap + col_gap * col_gap <= (reach * reach)[None, :]
    live = jnp.arange(KMAX, dtype=jnp.int32) < count
    return inside & live[None, :], live


def pad_tiles(resid):
    frames = resid.shape[2]
    blocks = resid.reshape(TILES, TILE_SIDE, TILE_SIDE, frames)
    field = jnp.transpose(blocks, (1, 0, 2, 3)).reshape(TILE_SIDE, TILES * TILE_SIDE, frames)
    padded = jnp.pad(field, ((CYCLE, CYCLE), (CYCLE, CYCLE), (0, 0)))
    pad_len = TILE_SIDE + 2 * CYCLE
    return [padded[:, tile_idx * TILE_SIDE:tile_idx * TILE_SIDE + pad_len, :] for tile_idx in range(TILES)]


def reference(movie, cycle_weights, footprints, traces, centre_row, centre_col, radius, comp_count):
    zero = jnp.zeros((), jnp.bfloat16)
    feet, lives, keeps, trace_now, den_a = [], [], [], [], []
    for tile_idx in range(TILES):
        keep, live = keep_mask(centre_row[tile_idx], centre_col[tile_idx], radius[tile_idx], comp_count[tile_idx])
        foot = jnp.where(keep, footprints[tile_idx], zero)
        feet.append(foot)
        keeps.append(keep)
        lives.append(live)
        trace_now.append(jnp.where(live[:, None], traces[tile_idx], zero))
        den_a.append(jnp.sum(jnp.square(foot.astype(jnp.float32)), axis=0) + RIDGE_TERM)
    movie_f = movie.astype(jnp.float32)
    backs = None
    for sweep in range(PASSES):
        prods = [jnp.dot(feet[tile_idx], trace_now[tile_idx], preferred_element_type=jnp.float32) for tile_idx in range(TILES)]
        resid = jnp.stack([(movie_f[tile_idx] - prods[tile_idx]).astype(jnp.bfloat16) for tile_idx in range(TILES)])
        windows = pad_tiles(resid)
        backs = [cycle_back(cycle_weights[tile_idx], windows[tile_idx]) for tile_idx in range(TILES)]
        updated = []
        for tile_idx in range(TILES):
            err = (prods[tile_idx] + backs[tile_idx].astype(jnp.float32) - movie_f[tile_idx]).astype(jnp.bfloat16)
            grad = lax.dot_general(feet[tile_idx], err, (((0,), (0,)), ((), ())), preferred_element_type=jnp.float32)
            moved = jnp.maximum(trace_now[tile_idx].astype(jnp.float32) - grad / den_a[tile_idx][:, None], 0.0)
            updated.append(jnp.where(lives[tile_idx][:, None], moved, 0.0).astype(jnp.bfloat16))
        trace_now = updated
    outs_a = []
    for tile_idx in range(TILES):
        prod = jnp.dot(feet[tile_idx], trace_now[tile_idx], preferred_element_type=jnp.float32)
        ferr = (prod + backs[tile_idx].astype(jnp.float32) - movie_f[tile_idx]).astype(jnp.bfloat16)
        grad_a = lax.dot_general(ferr, trace_now[tile_idx], (((1,), (1,)), ((), ())), preferred_element_type=jnp.float32)
        den_c = jnp.sum(jnp.square(trace_now[tile_idx].astype(jnp.float32)), axis=1) + RIDGE_TERM
        moved = jnp.maximum(feet[tile_idx].astype(jnp.float32) - grad_a / den_c[None, :], 0.0)
        outs_a.append(jnp.where(keeps[tile_idx], moved, 0.0).astype(jnp.bfloat16))
    return jnp.stack(outs_a), jnp.stack(trace_now)
```

```python
import functools

import jax
import jax.numpy as jnp
import numpy as np
from jax import lax
from jax.experimental import pallas as pl
from jax.experimental.pallas import tpu as pltpu
from jax.sharding import PartitionSpec as P

SIDE = 48
CYCLE = 8
WIDE = SIDE + 2 * CYCLE
FOLD = 24
PASSES = 2
RIDGE_TERM = 1.0
BLOCK = 4
SPAN = BLOCK + 2 * CYCLE
LANES = 128
F32 = jnp.float32
BF16 = jnp.bfloat16
MESH = pl.DeviceIdType.MESH


def cycle_offsets():
    found = []
    for row_step in range(-CYCLE, CYCLE + 1):
        for col_step in range(-CYCLE, CYCLE + 1):
            dist_sq = row_step * row_step + col_step * col_step
            if CYCLE * CYCLE <= dist_sq < (CYCLE + 1) * (CYCLE + 1):
                found.append((row_step, col_step))
    return found


def spread_tables():
    offsets = cycle_offsets()
    width = WIDE * (2 * CYCLE + 2)
    tables = np.zeros((2, len(offsets), width), np.float32)
    for index, (row_step, col_step) in enumerate(offsets):
        for odd in range(2):
            tables[odd, index, (row_step + CYCLE + odd) * WIDE + col_step + CYCLE] = 1.0
    return tables


def fold_columns(rows):
    return rows[:, :FOLD] + rows[:, FOLD:]


def kernel(
    n, s, shares,
    movie, weights, prints, traces, row_at, col_at, reach, count, tables,
    new_foot, new_trace,
    foot, band, pm, win, errs, backs, trace, gacc, inv_den, col_sq,
    halo_out, halo_in, part, own, arrived, energy_out, energy_in, gathered,
    halo_sems, part_sems, energy_sems, gather_sems,
):
    me = lax.axis_index("tm")
    tile = lax.axis_index("tile")
    frames = movie.shape[2]
    comps = prints.shape[2]
    blocks = SIDE // BLOCK

    barrier = pltpu.get_barrier_semaphore()
    pl.semaphore_signal(barrier, inc=1, device_id={"tile": 1 - tile}, device_id_type=MESH)

    def greet(t, carry):
        peer = lax.rem(me + 1 + t, n)
        pl.semaphore_signal(barrier, inc=1, device_id={"tm": peer}, device_id_type=MESH)
        return carry

    lax.fori_loop(0, n - 1, greet, 0)

    live_row = lax.broadcasted_iota(jnp.int32, (1, comps), 1) < count[0]
    bound = jnp.where(live_row, reach[...] * reach[...], -1)
    col_gap = lax.broadcasted_iota(jnp.int32, (SIDE, comps), 0) - col_at[...]
    col_sq[...] = col_gap * col_gap

    def mask_row(r, total):
        row_gap = r - row_at[...]
        keep = col_sq[...] <= bound - row_gap * row_gap
        kept = jnp.where(keep, prints[r].astype(F32), 0.0)
        foot[r] = kept.astype(BF16)
        return total + kept * kept

    total = lax.fori_loop(0, SIDE, mask_row, jnp.zeros((SIDE, comps), F32))
    den = jnp.sum(total, axis=0, keepdims=True) + RIDGE_TERM
    inv_den[...] = jnp.transpose(jnp.broadcast_to(1.0 / den, (LANES, comps)))
    live = lax.broadcasted_iota(jnp.int32, (comps, LANES), 0) < count[0]
    for q in range(frames // LANES):
        cols = slice(q * LANES, (q + 1) * LANES)
        trace[:, cols] = jnp.where(live, traces[:, cols].astype(F32), 0.0).astype(BF16)
    win[0:CYCLE] = jnp.zeros((CYCLE, WIDE, frames), BF16)
    win[CYCLE + SIDE : WIDE] = jnp.zeros((CYCLE, WIDE, frames), BF16)
    pl.semaphore_wait(barrier, n)

    def halo_copy(sweep):
        return pltpu.make_async_remote_copy(
            src_ref=halo_out.at[sweep],
            dst_ref=halo_in.at[sweep],
            send_sem=halo_sems.at[0, sweep],
            recv_sem=halo_sems.at[1, sweep],
            device_id={"tile": 1 - tile},
            device_id_type=MESH,
        )

    def build_band(b, carry):
        for i in range(BLOCK):
            spread = jnp.dot(weights[b * BLOCK + i], tables[i % 2], preferred_element_type=F32)
            first = (i // 2) * LANES
            rows = slice(i * SIDE, (i + 1) * SIDE)
            if first > 0:
                band[b, rows, 0:first] = jnp.zeros((SIDE, first), BF16)
            for q in range(spread.shape[1] // LANES):
                skewed = pltpu.roll(
                    spread[:, q * LANES : (q + 1) * LANES], 0, 1, stride=1, stride_axis=0
                )
                band[b, rows, first + q * LANES : first + (q + 1) * LANES] = skewed.astype(BF16)
            last = first + spread.shape[1]
            if last < SPAN * WIDE:
                band[b, rows, last:] = jnp.zeros((SIDE, SPAN * WIDE - last), BF16)
        return carry

    for sweep in range(PASSES):

        def residual(b, carry):
            rows = pl.ds(b * BLOCK, BLOCK)
            prod = jnp.dot(
                foot[rows].reshape(BLOCK * SIDE, comps), trace[...], preferred_element_type=F32
            )
            diff = prod.reshape(BLOCK, SIDE, frames) - movie[rows].astype(F32)
            pm[rows] = diff
            edge = jnp.where(tile == 0, -diff[:, SIDE - CYCLE :], -diff[:, :CYCLE])
            halo_out[sweep, b] = edge.reshape(BLOCK * CYCLE, frames).astype(BF16)
            return carry

        lax.fori_loop(0, blocks, residual, 0)
        copy = halo_copy(sweep)
        copy.start()
        if sweep == 0:
            lax.fori_loop(0, blocks, build_band, 0)
        copy.wait_recv()

        def fill(b, carry):
            rows = pl.ds(b * BLOCK, BLOCK)
            edge = halo_in[sweep, b].astype(F32).reshape(BLOCK, CYCLE, frames)
            low = jnp.where(tile == 0, 0.0, edge)
            high = jnp.where(tile == 0, edge, 0.0)
            whole = jnp.concatenate([low, -pm[rows], high], axis=1)
            win[pl.ds(CYCLE + b * BLOCK, BLOCK)] = whole.astype(BF16)
            return carry

        lax.fori_loop(0, blocks, fill, 0)

        def background(b, carry):
            rows = pl.ds(b * BLOCK, BLOCK)
            seen = win[pl.ds(b * BLOCK, SPAN)].reshape(SPAN * WIDE, frames)
            back = jnp.dot(band[b], seen, preferred_element_type=F32).astype(BF16)
            back = back.reshape(BLOCK, SIDE, frames)
            if sweep == PASSES - 1:
                backs[rows] = back
            errs[rows] = (pm[rows] + back.astype(F32)).astype(BF16)
            return carry

        lax.fori_loop(0, blocks, background, 0)

        depth = 16
        gacc[...] = jnp.zeros_like(gacc)

        def descend(j, carry):
            rows = pl.ds(j * depth, depth)
            gacc[...] += lax.dot_general(
                foot[rows].reshape(depth * SIDE, comps),
                errs[rows].reshape(depth * SIDE, frames),
                (((0,), (0,)), ((), ())),
                preferred_element_type=F32,
            )
            return carry

        lax.fori_loop(0, SIDE // depth, descend, 0)
        for q in range(frames // LANES):
            cols = slice(q * LANES, (q + 1) * LANES)
            moved = jnp.maximum(trace[:, cols].astype(F32) - gacc[:, cols] * inv_den[...], 0.0)
            trace[:, cols] = jnp.where(live, moved, 0.0).astype(BF16)

    new_trace[...] = trace[...]
    squares = jnp.zeros((comps, LANES), F32)
    for q in range(frames // LANES):
        now = trace[:, q * LANES : (q + 1) * LANES].astype(F32)
        squares = squares + now * now
    energy = jnp.sum(jnp.transpose(squares), axis=0, keepdims=True)
    energy_out[...] = jnp.broadcast_to(energy, energy_out.shape)

    def energy_copy(peer, sender):
        return pltpu.make_async_remote_copy(
            src_ref=energy_out,
            dst_ref=energy_in.at[sender],
            send_sem=energy_sems.at[0, peer],
            recv_sem=energy_sems.at[1, sender],
            device_id={"tm": peer},
            device_id_type=MESH,
        )

    def part_copy(peer, sender):
        return pltpu.make_async_remote_copy(
            src_ref=part.at[peer],
            dst_ref=arrived.at[sender],
            send_sem=part_sems.at[0, peer],
            recv_sem=part_sems.at[1, sender],
            device_id={"tm": peer},
            device_id_type=MESH,
        )

    def gather_copy(peer, sender):
        return pltpu.make_async_remote_copy(
            src_ref=gathered.at[sender],
            dst_ref=gathered.at[sender],
            send_sem=gather_sems.at[0, peer],
            recv_sem=gather_sems.at[1, sender],
            device_id={"tm": peer},
            device_id_type=MESH,
        )

    def owns(index, do):
        if shares == n:
            do()
        else:
            pl.when(index < shares)(do)

    def over_peers(do):
        def step(t, carry):
            do(lax.rem(me + 1 + t, n))
            return carry

        lax.fori_loop(0, n - 1, step, 0)

    over_peers(lambda peer: owns(peer, lambda: energy_copy(peer, me).start()))

    def share_of(share):
        top, low = pl.ds(share * s, s), pl.ds(FOLD + share * s, s)
        feet = jnp.concatenate([foot[top], foot[low]], axis=0).reshape(2 * s * SIDE, comps)
        prod = jnp.dot(feet, trace[...], preferred_element_type=F32)
        back = jnp.concatenate([backs[top], backs[low]], axis=0).reshape(2 * s * SIDE, frames)
        seen = jnp.concatenate([movie[top], movie[low]], axis=0).reshape(2 * s * SIDE, frames)
        ferr = (prod + back.astype(F32) - seen.astype(F32)).astype(BF16)
        grad = lax.dot_general(
            ferr, trace[...], (((1,), (1,)), ((), ())), preferred_element_type=F32
        )
        grad = jnp.where(feet.astype(F32) > 0.0, grad, 0.0).reshape(2 * s, SIDE, comps)
        return fold_columns(grad[:s] + grad[s:]).reshape(s * FOLD, comps)

    def send_share(share):
        part[share] = share_of(share).astype(BF16)
        part_copy(share, me).start()

    over_peers(lambda peer: owns(peer, lambda: send_share(peer)))

    def settle():
        own[...] = share_of(me)
        energy_in[me] = energy_out[...]

        def take(peer):
            energy_copy(me, peer).wait_recv()
            part_copy(me, peer).wait_recv()
            own[...] += arrived[peer].astype(F32)
            energy_in[me] += energy_in[peer]

        over_peers(take)
        den_c = energy_in[me][:1] + RIDGE_TERM
        top, low = pl.ds(me * s, s), pl.ds(FOLD + me * s, s)
        feet = fold_columns(foot[top].astype(F32) + foot[low].astype(F32)).reshape(s * FOLD, comps)
        gathered[me] = jnp.maximum(feet - own[...] / den_c, 0.0).astype(BF16)
        over_peers(lambda peer: gather_copy(peer, me).start())

    owns(me, settle)

    def unfold(share):
        values = gathered[share].astype(F32).reshape(s, FOLD, comps)
        values = jnp.concatenate([values, values], axis=1)
        for half in range(2):
            rows = pl.ds(half * FOLD + share * s, s)
            new_foot[rows] = jnp.where(foot[rows].astype(F32) > 0.0, values, 0.0).astype(BF16)

    owns(me, lambda: unfold(me))

    def receive(peer):
        gather_copy(me, peer).wait_recv()
        unfold(peer)

    over_peers(lambda peer: owns(peer, lambda: receive(peer)))

    for sweep in range(PASSES):
        halo_copy(sweep).wait_send()

    def drain(peer):
        owns(peer, lambda: energy_copy(peer, me).wait_send())
        owns(peer, lambda: part_copy(peer, me).wait_send())
        owns(me, lambda: gather_copy(peer, me).wait_send())

    over_peers(drain)


def shards(movie, cycle_weights, footprints, traces, centre_row, centre_col, radius, comp_count):
    n = lax.axis_size("tm")
    frames = movie.shape[2]
    comps = footprints.shape[2]
    s = -(-FOLD // n)
    while FOLD % s:
        s += 1
    shares = FOLD // s
    blocks = SIDE // BLOCK
    tables = jnp.asarray(spread_tables(), BF16)
    vmem = pl.BlockSpec(memory_space=pltpu.VMEM)
    smem = pl.BlockSpec(memory_space=pltpu.SMEM)
    new_foot, new_trace = pl.pallas_call(
        functools.partial(kernel, n, s, shares),
        out_shape=(
            jax.ShapeDtypeStruct((SIDE, SIDE, comps), BF16),
            jax.ShapeDtypeStruct((comps, frames), BF16),
        ),
        in_specs=[vmem] * 7 + [smem, vmem],
        out_specs=(vmem, vmem),
        scratch_shapes=[
            pltpu.VMEM((SIDE, SIDE, comps), BF16),
            pltpu.VMEM((blocks, BLOCK * SIDE, SPAN * WIDE), BF16),
            pltpu.VMEM((SIDE, SIDE, frames), F32),
            pltpu.VMEM((WIDE, WIDE, frames), BF16),
            pltpu.VMEM((SIDE, SIDE, frames), BF16),
            pltpu.VMEM((SIDE, SIDE, frames), BF16),
            pltpu.VMEM((comps, frames), BF16),
            pltpu.VMEM((comps, frames), F32),
            pltpu.VMEM((comps, LANES), F32),
            pltpu.VMEM((SIDE, comps), jnp.int32),
            pltpu.VMEM((PASSES, blocks, BLOCK * CYCLE, frames), BF16),
            pltpu.VMEM((PASSES, blocks, BLOCK * CYCLE, frames), BF16),
            pltpu.VMEM((n, s * FOLD, comps), BF16),
            pltpu.VMEM((s * FOLD, comps), F32),
            pltpu.VMEM((n, s * FOLD, comps), BF16),
            pltpu.VMEM((8, comps), F32),
            pltpu.VMEM((n, 8, comps), F32),
            pltpu.VMEM((n, s * FOLD, comps), BF16),
            pltpu.SemaphoreType.DMA((2, PASSES)),
            pltpu.SemaphoreType.DMA((2, n)),
            pltpu.SemaphoreType.DMA((2, n)),
            pltpu.SemaphoreType.DMA((2, n)),
        ],
        compiler_params=pltpu.CompilerParams(
            collective_id=0, has_side_effects=True, vmem_limit_bytes=60 * 1024 * 1024
        ),
    )(
        movie.reshape(SIDE, SIDE, frames),
        cycle_weights.reshape(SIDE, SIDE, -1),
        footprints.reshape(SIDE, SIDE, comps),
        traces.reshape(comps, frames),
        centre_row,
        centre_col,
        radius,
        comp_count,
        tables,
    )
    return (new_foot.reshape(1, SIDE * SIDE, comps), new_trace[None])


def solution(mesh):
    in_specs = (
        P(("groups", "tile"), None, "tm"),
        P(("groups", "tile"), None, None),
        P(("groups", "tile"), None, None),
        P(("groups", "tile"), None, "tm"),
        P(("groups", "tile"), None),
        P(("groups", "tile"), None),
        P(("groups", "tile"), None),
        P(("groups", "tile")),
    )
    out_specs = (P(("groups", "tile"), None, None), P(("groups", "tile"), None, "tm"))
    return jax.shard_map(shards, mesh=mesh, in_specs=in_specs, out_specs=out_specs, check_vma=False)
```

```python
import functools

import jax
import jax.numpy as jnp
import numpy as np
from jax import lax
from jax.experimental import pallas as pl
from jax.experimental.pallas import tpu as pltpu
from jax.sharding import PartitionSpec as P

SIDE = 48
CYCLE = 8
WIDE = SIDE + 2 * CYCLE
FOLD_ROWS = 16
FOLD = 24
HALF = FOLD // 2
PASSES = 2
RIDGE_TERM = 1.0
BLOCK = 8
DEPTH = 16
SPAN = BLOCK + 2 * CYCLE
LANES = 128
F32 = jnp.float32
BF16 = jnp.bfloat16
MESH = pl.DeviceIdType.MESH


def cycle_offsets():
    found = []
    for row_step in range(-CYCLE, CYCLE + 1):
        for col_step in range(-CYCLE, CYCLE + 1):
            dist_sq = row_step * row_step + col_step * col_step
            if CYCLE * CYCLE <= dist_sq < (CYCLE + 1) * (CYCLE + 1):
                found.append((row_step, col_step))
    return found


def spread_tables():
    offsets = cycle_offsets()
    width = WIDE * (2 * CYCLE + 2)
    tables = np.zeros((2, len(offsets), width), np.float32)
    for index, (row_step, col_step) in enumerate(offsets):
        for odd in range(2):
            tables[odd, index, (row_step + CYCLE + odd) * WIDE + col_step + CYCLE] = 1.0
    return tables


def swap_halves(rows):
    return jnp.concatenate([rows[:, HALF:], rows[:, :HALF]], axis=1)


def fold(rows, s):
    rows = rows[:, :FOLD] + rows[:, FOLD:]
    rows = rows[:s] + swap_halves(rows[s : 2 * s]) + rows[2 * s :]
    return rows.reshape(s * FOLD, rows.shape[2])


def kernel(
    n, s, shares,
    movie, stored, prints, traces, row_at, col_at, reach, count, tables,
    new_foot, new_trace,
    weights, foot, band, pm, win, errs, backs, trace, gacc, inv_den, col_sq,
    halo_out, halo_in, part, own, arrived, energy_out, energy_in, gathered,
    halo_sems, part_sems, energy_sems, gather_sems,
):
    me = lax.axis_index("tm")
    tile = lax.axis_index("tile")
    frames = movie.shape[2]
    comps = prints.shape[2]
    blocks = SIDE // BLOCK

    barrier = pltpu.get_barrier_semaphore()
    pl.semaphore_signal(barrier, inc=1, device_id={"tile": 1 - tile}, device_id_type=MESH)

    def greet(t, carry):
        peer = lax.rem(me + 1 + t, n)
        pl.semaphore_signal(barrier, inc=1, device_id={"tm": peer}, device_id_type=MESH)
        return carry

    lax.fori_loop(0, n - 1, greet, 0)

    live_row = lax.broadcasted_iota(jnp.int32, (1, comps), 1) < count[0]
    bound = jnp.where(live_row, reach[...] * reach[...], -1)
    col_gap = lax.broadcasted_iota(jnp.int32, (SIDE, comps), 0) - col_at[...]
    col_sq[...] = col_gap * col_gap

    def mask_row(r, total):
        row_gap = r - row_at[...]
        keep = col_sq[...] <= bound - row_gap * row_gap
        kept = jnp.where(keep, prints[r].astype(F32), 0.0)
        foot[r] = kept.astype(BF16)
        return total + kept * kept

    total = lax.fori_loop(0, SIDE, mask_row, jnp.zeros((SIDE, comps), F32))
    den = jnp.sum(total, axis=0, keepdims=True) + RIDGE_TERM
    inv_den[...] = jnp.transpose(jnp.broadcast_to(1.0 / den, (LANES, comps)))
    live = lax.broadcasted_iota(jnp.int32, (comps, LANES), 0) < count[0]
    for q in range(frames // LANES):
        cols = slice(q * LANES, (q + 1) * LANES)
        trace[:, cols] = jnp.where(live, traces[:, cols].astype(F32), 0.0).astype(BF16)
    pixels = BLOCK * SIDE
    for b in range(blocks):
        turned = jnp.transpose(stored[:, b * pixels : (b + 1) * pixels].astype(F32))
        weights[b * BLOCK : (b + 1) * BLOCK] = turned.astype(BF16).reshape(BLOCK, SIDE, -1)
    pl.semaphore_wait(barrier, n)

    def halo_copy(sweep):
        return pltpu.make_async_remote_copy(
            src_ref=halo_out.at[sweep],
            dst_ref=halo_in.at[sweep],
            send_sem=halo_sems.at[0, sweep],
            recv_sem=halo_sems.at[1, sweep],
            device_id={"tile": 1 - tile},
            device_id_type=MESH,
        )

    def build_band(b, carry):
        for i in range(BLOCK):
            spread = jnp.dot(weights[b * BLOCK + i], tables[i % 2], preferred_element_type=F32)
            first = (i // 2) * LANES
            rows = slice(i * SIDE, (i + 1) * SIDE)
            if first > 0:
                band[b, rows, 0:first] = jnp.zeros((SIDE, first), BF16)
            for q in range(spread.shape[1] // LANES):
                skewed = pltpu.roll(
                    spread[:, q * LANES : (q + 1) * LANES], 0, 1, stride=1, stride_axis=0
                )
                band[b, rows, first + q * LANES : first + (q + 1) * LANES] = skewed.astype(BF16)
            last = first + spread.shape[1]
            if last < SPAN * WIDE:
                band[b, rows, last:] = jnp.zeros((SIDE, SPAN * WIDE - last), BF16)
        return carry

    for sweep in range(PASSES):

        def residual(b, carry):
            rows = pl.ds(b * DEPTH, DEPTH)
            prod = jnp.dot(
                foot[rows].reshape(DEPTH * SIDE, comps), trace[...], preferred_element_type=F32
            )
            diff = prod.reshape(DEPTH, SIDE, frames) - movie[rows].astype(F32)
            pm[rows] = diff
            edge = jnp.where(tile == 0, -diff[:, SIDE - CYCLE :], -diff[:, :CYCLE])
            edge = edge.reshape(DEPTH * CYCLE, frames).astype(BF16)
            halo_out[sweep, pl.ds(b * DEPTH * CYCLE, DEPTH * CYCLE)] = edge
            return carry

        lax.fori_loop(0, SIDE // DEPTH, residual, 0)
        copy = halo_copy(sweep)
        copy.start()
        if sweep == 0:
            lax.fori_loop(0, blocks, build_band, 0)
        copy.wait_recv()

        def fill(b, carry):
            rows = pl.ds(b * BLOCK, BLOCK)
            edge = halo_in[sweep, pl.ds(b * BLOCK * CYCLE, BLOCK * CYCLE)]
            edge = edge.astype(F32).reshape(BLOCK, CYCLE, frames)
            low = jnp.where(tile == 0, 0.0, edge)
            high = jnp.where(tile == 0, edge, 0.0)
            whole = jnp.concatenate([low, -pm[rows], high], axis=1)
            win[rows] = whole.astype(BF16)
            return carry

        lax.fori_loop(0, blocks, fill, 0)

        for b in range(blocks):
            rows = slice(b * BLOCK, (b + 1) * BLOCK)
            first = b * BLOCK - CYCLE
            low, high = max(first, 0), min(first + SPAN, SIDE)
            seen = win[low:high].reshape((high - low) * WIDE, frames)
            taps = band[b, :, (low - first) * WIDE : (high - first) * WIDE]
            back = jnp.dot(taps, seen, preferred_element_type=F32).astype(BF16)
            back = back.reshape(BLOCK, SIDE, frames)
            if sweep == PASSES - 1:
                backs[rows] = back
            errs[rows] = (pm[rows] + back.astype(F32)).astype(BF16)

        gacc[...] = jnp.zeros_like(gacc)

        def descend(j, carry):
            rows = pl.ds(j * DEPTH, DEPTH)
            gacc[...] += lax.dot_general(
                foot[rows].reshape(DEPTH * SIDE, comps),
                errs[rows].reshape(DEPTH * SIDE, frames),
                (((0,), (0,)), ((), ())),
                preferred_element_type=F32,
            )
            return carry

        lax.fori_loop(0, SIDE // DEPTH, descend, 0)
        for q in range(frames // LANES):
            cols = slice(q * LANES, (q + 1) * LANES)
            moved = jnp.maximum(trace[:, cols].astype(F32) - gacc[:, cols] * inv_den[...], 0.0)
            trace[:, cols] = jnp.where(live, moved, 0.0).astype(BF16)

    new_trace[...] = trace[...]
    squares = jnp.zeros((comps, LANES), F32)
    for q in range(frames // LANES):
        now = trace[:, q * LANES : (q + 1) * LANES].astype(F32)
        squares = squares + now * now
    energy = jnp.sum(jnp.transpose(squares), axis=0, keepdims=True)
    energy_out[...] = jnp.broadcast_to(energy, energy_out.shape)

    def energy_copy(peer, sender):
        return pltpu.make_async_remote_copy(
            src_ref=energy_out,
            dst_ref=energy_in.at[sender],
            send_sem=energy_sems.at[0, peer],
            recv_sem=energy_sems.at[1, sender],
            device_id={"tm": peer},
            device_id_type=MESH,
        )

    def part_copy(peer, sender):
        return pltpu.make_async_remote_copy(
            src_ref=part.at[peer],
            dst_ref=arrived.at[sender],
            send_sem=part_sems.at[0, peer],
            recv_sem=part_sems.at[1, sender],
            device_id={"tm": peer},
            device_id_type=MESH,
        )

    def gather_copy(peer, sender):
        return pltpu.make_async_remote_copy(
            src_ref=gathered.at[sender],
            dst_ref=gathered.at[sender],
            send_sem=gather_sems.at[0, peer],
            recv_sem=gather_sems.at[1, sender],
            device_id={"tm": peer},
            device_id_type=MESH,
        )

    def owns(index, do):
        if shares == n:
            do()
        else:
            pl.when(index < shares)(do)

    def over_peers(do):
        def step(t, carry):
            do(lax.rem(me + 1 + t, n))
            return carry

        lax.fori_loop(0, n - 1, step, 0)

    over_peers(lambda peer: owns(peer, lambda: energy_copy(peer, me).start()))

    def rows_of(ref, share):
        return [ref[pl.ds(a * FOLD_ROWS + share * s, s)] for a in range(SIDE // FOLD_ROWS)]

    def share_of(share):
        held = SIDE // FOLD_ROWS * s * SIDE
        feet = jnp.concatenate(rows_of(foot, share), axis=0).reshape(held, comps)
        prod = jnp.dot(feet, trace[...], preferred_element_type=F32)
        back = jnp.concatenate(rows_of(backs, share), axis=0).reshape(held, frames)
        seen = jnp.concatenate(rows_of(movie, share), axis=0).reshape(held, frames)
        ferr = (prod + back.astype(F32) - seen.astype(F32)).astype(BF16)
        grad = lax.dot_general(
            ferr, trace[...], (((1,), (1,)), ((), ())), preferred_element_type=F32
        )
        grad = jnp.where(feet.astype(F32) > 0.0, grad, 0.0)
        return fold(grad.reshape(held // SIDE, SIDE, comps), s)

    def send_share(share):
        part[share] = share_of(share).astype(BF16)
        part_copy(share, me).start()

    over_peers(lambda peer: owns(peer, lambda: send_share(peer)))

    def settle():
        own[...] = share_of(me)
        energy_in[me] = energy_out[...]

        def take(peer):
            energy_copy(me, peer).wait_recv()
            part_copy(me, peer).wait_recv()
            own[...] += arrived[peer].astype(F32)
            energy_in[me] += energy_in[peer]

        over_peers(take)
        den_c = energy_in[me][:1] + RIDGE_TERM
        feet = fold(jnp.concatenate(rows_of(foot, me), axis=0).astype(F32), s)
        gathered[me] = jnp.maximum(feet - own[...] / den_c, 0.0).astype(BF16)
        over_peers(lambda peer: gather_copy(peer, me).start())

    owns(me, settle)

    def unfold(share):
        values = gathered[share].astype(F32).reshape(s, FOLD, comps)
        turned = swap_halves(values)
        values = jnp.concatenate([values, values], axis=1)
        turned = jnp.concatenate([turned, turned], axis=1)
        for a in range(SIDE // FOLD_ROWS):
            rows = pl.ds(a * FOLD_ROWS + share * s, s)
            new_foot[rows] = jnp.where(foot[rows].astype(F32) > 0.0, (values, turned)[a % 2], 0.0).astype(BF16)

    owns(me, lambda: unfold(me))

    def receive(peer):
        gather_copy(me, peer).wait_recv()
        unfold(peer)

    over_peers(lambda peer: owns(peer, lambda: receive(peer)))

    for sweep in range(PASSES):
        halo_copy(sweep).wait_send()

    def drain(peer):
        owns(peer, lambda: energy_copy(peer, me).wait_send())
        owns(peer, lambda: part_copy(peer, me).wait_send())
        owns(me, lambda: gather_copy(peer, me).wait_send())

    over_peers(drain)


def shards(movie, cycle_weights, footprints, traces, centre_row, centre_col, radius, comp_count):
    n = lax.axis_size("tm")
    frames = movie.shape[2]
    comps = footprints.shape[2]
    s = -(-FOLD_ROWS // n)
    while FOLD_ROWS % s:
        s += 1
    shares = FOLD_ROWS // s
    blocks = SIDE // BLOCK
    tables = jnp.asarray(spread_tables(), BF16)
    vmem = pl.BlockSpec(memory_space=pltpu.VMEM)
    smem = pl.BlockSpec(memory_space=pltpu.SMEM)
    new_foot, new_trace = pl.pallas_call(
        functools.partial(kernel, n, s, shares),
        out_shape=(
            jax.ShapeDtypeStruct((SIDE, SIDE, comps), BF16),
            jax.ShapeDtypeStruct((comps, frames), BF16),
        ),
        in_specs=[vmem] * 7 + [smem, vmem],
        out_specs=(vmem, vmem),
        scratch_shapes=[
            pltpu.VMEM((SIDE, SIDE, cycle_weights.shape[2]), BF16),
            pltpu.VMEM((SIDE, SIDE, comps), BF16),
            pltpu.VMEM((blocks, BLOCK * SIDE, SPAN * WIDE), BF16),
            pltpu.VMEM((SIDE, SIDE, frames), F32),
            pltpu.VMEM((SIDE, WIDE, frames), BF16),
            pltpu.VMEM((SIDE, SIDE, frames), BF16),
            pltpu.VMEM((SIDE, SIDE, frames), BF16),
            pltpu.VMEM((comps, frames), BF16),
            pltpu.VMEM((comps, frames), F32),
            pltpu.VMEM((comps, LANES), F32),
            pltpu.VMEM((SIDE, comps), jnp.int32),
            pltpu.VMEM((PASSES, SIDE * CYCLE, frames), BF16),
            pltpu.VMEM((PASSES, SIDE * CYCLE, frames), BF16),
            pltpu.VMEM((n, s * FOLD, comps), BF16),
            pltpu.VMEM((s * FOLD, comps), F32),
            pltpu.VMEM((n, s * FOLD, comps), BF16),
            pltpu.VMEM((8, comps), F32),
            pltpu.VMEM((n, 8, comps), F32),
            pltpu.VMEM((n, s * FOLD, comps), BF16),
            pltpu.SemaphoreType.DMA((2, PASSES)),
            pltpu.SemaphoreType.DMA((2, n)),
            pltpu.SemaphoreType.DMA((2, n)),
            pltpu.SemaphoreType.DMA((2, n)),
        ],
        compiler_params=pltpu.CompilerParams(
            collective_id=0, has_side_effects=True, vmem_limit_bytes=60 * 1024 * 1024
        ),
    )(
        movie.reshape(SIDE, SIDE, frames),
        jnp.transpose(cycle_weights[0]),
        footprints.reshape(SIDE, SIDE, comps),
        traces.reshape(comps, frames),
        centre_row,
        centre_col,
        radius,
        comp_count,
        tables,
    )
    return (new_foot.reshape(1, SIDE * SIDE, comps), new_trace[None])


def solution(mesh):
    in_specs = (
        P(("groups", "tile"), None, "tm"),
        P(("groups", "tile"), None, None),
        P(("groups", "tile"), None, None),
        P(("groups", "tile"), None, "tm"),
        P(("groups", "tile"), None),
        P(("groups", "tile"), None),
        P(("groups", "tile"), None),
        P(("groups", "tile")),
    )
    out_specs = (P(("groups", "tile"), None, None), P(("groups", "tile"), None, "tm"))
    return jax.shard_map(shards, mesh=mesh, in_specs=in_specs, out_specs=out_specs, check_vma=False)
```

```python
import functools

import jax
import jax.numpy as jnp
import numpy as np
from jax import lax
from jax.experimental import pallas as pl
from jax.experimental.pallas import tpu as pltpu
from jax.sharding import PartitionSpec as P

SIDE = 48
CYCLE = 8
WIDE = SIDE + 2 * CYCLE
FOLD_ROWS = 16
FOLD = 24
HALF = FOLD // 2
PASSES = 2
RIDGE_TERM = 1.0
BLOCK = 8
DEPTH = 16
SPAN = BLOCK + 2 * CYCLE
LANES = 128
F32 = jnp.float32
BF16 = jnp.bfloat16
MESH = pl.DeviceIdType.MESH


def cycle_offsets():
    found = []
    for row_step in range(-CYCLE, CYCLE + 1):
        for col_step in range(-CYCLE, CYCLE + 1):
            dist_sq = row_step * row_step + col_step * col_step
            if CYCLE * CYCLE <= dist_sq < (CYCLE + 1) * (CYCLE + 1):
                found.append((row_step, col_step))
    return found


def spread_tables():
    offsets = cycle_offsets()
    width = WIDE * (2 * CYCLE + 2)
    tables = np.zeros((2, len(offsets), width), np.float32)
    for index, (row_step, col_step) in enumerate(offsets):
        for odd in range(2):
            tables[odd, index, (row_step + CYCLE + odd) * WIDE + col_step + CYCLE] = 1.0
    return tables


def swap_halves(rows):
    return jnp.concatenate([rows[:, HALF:], rows[:, :HALF]], axis=1)


def fold(rows, s):
    rows = rows[:, :FOLD] + rows[:, FOLD:]
    rows = rows[:s] + swap_halves(rows[s : 2 * s]) + rows[2 * s :]
    return rows.reshape(s * FOLD, rows.shape[2])


def kernel(
    n, s,
    movie, stored, prints, traces, row_at, col_at, reach, count, tables,
    foot_out, trace_out, packed_out,
    feet_edge, seen_edge, weights, foot, band, pm, win, errs, backs, trace, gacc, inv_den, col_sq,
    halo_out, halo_in, part, own, arrived, energy_out, energy_in, gathered,
    halo_sems, part_sems, energy_sems, gather_sems, relay_sems, out_sems, share_sems,
):
    me = lax.axis_index("tm")
    tile = lax.axis_index("tile")
    frames = movie.shape[2]
    comps = prints.shape[2]
    blocks = SIDE // BLOCK

    barrier = pltpu.get_barrier_semaphore()
    pl.semaphore_signal(barrier, inc=1, device_id={"tile": 1 - tile}, device_id_type=MESH)

    def greet(t, carry):
        peer = lax.rem(me + 1 + t, n)
        pl.semaphore_signal(barrier, inc=1, device_id={"tm": peer}, device_id_type=MESH)
        return carry

    lax.fori_loop(0, n - 1, greet, 0)

    live_row = lax.broadcasted_iota(jnp.int32, (1, comps), 1) < count[0]
    bound = jnp.where(live_row, reach[...] * reach[...], -1)
    col_gap = lax.broadcasted_iota(jnp.int32, (SIDE, comps), 0) - col_at[...]
    col_sq[...] = col_gap * col_gap

    def mask_row(r, total):
        row_gap = r - row_at[...]
        keep = col_sq[...] <= bound - row_gap * row_gap
        kept = jnp.where(keep, prints[r].astype(F32), 0.0)
        foot[r] = kept.astype(BF16)
        return total + kept * kept

    total = lax.fori_loop(0, SIDE, mask_row, jnp.zeros((SIDE, comps), F32))
    den = jnp.sum(total, axis=0, keepdims=True) + RIDGE_TERM
    inv_den[...] = jnp.transpose(jnp.broadcast_to(1.0 / den, (LANES, comps)))
    live = lax.broadcasted_iota(jnp.int32, (comps, LANES), 0) < count[0]
    for q in range(frames // LANES):
        cols = slice(q * LANES, (q + 1) * LANES)
        trace[:, cols] = jnp.where(live, traces[:, cols].astype(F32), 0.0).astype(BF16)

    def cut_edge(j, carry):
        rows = pl.ds(j * DEPTH, DEPTH)
        spots = pl.ds(j * DEPTH * CYCLE, DEPTH * CYCLE)
        for ref, edge in ((foot, feet_edge), (movie, seen_edge)):
            whole = ref[rows].astype(F32)
            cut = jnp.where(tile == 0, whole[:, SIDE - CYCLE :], whole[:, :CYCLE])
            edge[spots] = cut.reshape(DEPTH * CYCLE, ref.shape[2]).astype(BF16)
        return carry

    lax.fori_loop(0, SIDE // DEPTH, cut_edge, 0)
    pixels = BLOCK * SIDE
    for b in range(blocks):
        turned = jnp.transpose(stored[:, b * pixels : (b + 1) * pixels].astype(F32))
        weights[b * BLOCK : (b + 1) * BLOCK] = turned.astype(BF16).reshape(BLOCK, SIDE, -1)
    pl.semaphore_wait(barrier, n)

    def halo_copy(sweep):
        return pltpu.make_async_remote_copy(
            src_ref=halo_out.at[sweep],
            dst_ref=halo_in.at[sweep],
            send_sem=halo_sems.at[0, sweep],
            recv_sem=halo_sems.at[1, sweep],
            device_id={"tile": 1 - tile},
            device_id_type=MESH,
        )

    def build_band(b, carry):
        for i in range(BLOCK):
            spread = jnp.dot(weights[b * BLOCK + i], tables[i % 2], preferred_element_type=F32)
            first = (i // 2) * LANES
            rows = slice(i * SIDE, (i + 1) * SIDE)
            if first > 0:
                band[b, rows, 0:first] = jnp.zeros((SIDE, first), BF16)
            for q in range(spread.shape[1] // LANES):
                skewed = pltpu.roll(
                    spread[:, q * LANES : (q + 1) * LANES], 0, 1, stride=1, stride_axis=0
                )
                band[b, rows, first + q * LANES : first + (q + 1) * LANES] = skewed.astype(BF16)
            last = first + spread.shape[1]
            if last < SPAN * WIDE:
                band[b, rows, last:] = jnp.zeros((SIDE, SPAN * WIDE - last), BF16)
        return carry

    foot_copy = pltpu.make_async_copy(foot, foot_out, out_sems.at[0])
    trace_copy = pltpu.make_async_copy(trace, trace_out, out_sems.at[1])

    for sweep in range(PASSES):

        def residual(b, carry):
            rows = pl.ds(b * DEPTH, DEPTH)
            prod = jnp.dot(
                foot[rows].reshape(DEPTH * SIDE, comps), trace[...], preferred_element_type=F32
            )
            diff = prod.reshape(DEPTH, SIDE, frames) - movie[rows].astype(F32)
            pm[rows] = diff
            return carry

        ahead = jnp.dot(feet_edge[...], trace[...], preferred_element_type=F32)
        halo_out[sweep] = (seen_edge[...].astype(F32) - ahead).astype(BF16)
        copy = halo_copy(sweep)
        copy.start()
        lax.fori_loop(0, SIDE // DEPTH, residual, 0)
        if sweep == 0:
            lax.fori_loop(0, blocks, build_band, 0)
            foot_copy.start()
        copy.wait_recv()

        def fill(b, carry):
            rows = pl.ds(b * BLOCK, BLOCK)
            edge = halo_in[sweep, pl.ds(b * BLOCK * CYCLE, BLOCK * CYCLE)]
            edge = edge.astype(F32).reshape(BLOCK, CYCLE, frames)
            low = jnp.where(tile == 0, 0.0, edge)
            high = jnp.where(tile == 0, edge, 0.0)
            whole = jnp.concatenate([low, -pm[rows], high], axis=1)
            win[rows] = whole.astype(BF16)
            return carry

        lax.fori_loop(0, blocks, fill, 0)

        for b in range(blocks):
            rows = slice(b * BLOCK, (b + 1) * BLOCK)
            first = b * BLOCK - CYCLE
            low, high = max(first, 0), min(first + SPAN, SIDE)
            seen = win[low:high].reshape((high - low) * WIDE, frames)
            taps = band[b, :, (low - first) * WIDE : (high - first) * WIDE]
            back = jnp.dot(taps, seen, preferred_element_type=F32).astype(BF16)
            back = back.reshape(BLOCK, SIDE, frames)
            if sweep == PASSES - 1:
                backs[rows] = back
            errs[rows] = (pm[rows] + back.astype(F32)).astype(BF16)

        gacc[...] = jnp.zeros_like(gacc)

        def descend(j, carry):
            rows = pl.ds(j * DEPTH, DEPTH)
            gacc[...] += lax.dot_general(
                foot[rows].reshape(DEPTH * SIDE, comps),
                errs[rows].reshape(DEPTH * SIDE, frames),
                (((0,), (0,)), ((), ())),
                preferred_element_type=F32,
            )
            return carry

        lax.fori_loop(0, SIDE // DEPTH, descend, 0)
        for q in range(frames // LANES):
            cols = slice(q * LANES, (q + 1) * LANES)
            moved = jnp.maximum(trace[:, cols].astype(F32) - gacc[:, cols] * inv_den[...], 0.0)
            trace[:, cols] = jnp.where(live, moved, 0.0).astype(BF16)

    squares = jnp.zeros((comps, LANES), F32)
    for q in range(frames // LANES):
        now = trace[:, q * LANES : (q + 1) * LANES].astype(F32)
        squares = squares + now * now
    energy = jnp.sum(jnp.transpose(squares), axis=0, keepdims=True)
    energy_out[...] = jnp.broadcast_to(energy, energy_out.shape)

    def energy_copy(peer, sender):
        return pltpu.make_async_remote_copy(
            src_ref=energy_out,
            dst_ref=energy_in.at[sender],
            send_sem=energy_sems.at[0, peer],
            recv_sem=energy_sems.at[1, sender],
            device_id={"tm": peer},
            device_id_type=MESH,
        )

    def part_copy(peer, sender):
        return pltpu.make_async_remote_copy(
            src_ref=part.at[peer],
            dst_ref=arrived.at[sender],
            send_sem=part_sems.at[0, peer],
            recv_sem=part_sems.at[1, sender],
            device_id={"tm": peer},
            device_id_type=MESH,
        )

    def gather_copy(peer, sender):
        return pltpu.make_async_remote_copy(
            src_ref=gathered.at[sender],
            dst_ref=gathered.at[sender],
            send_sem=gather_sems.at[0, peer],
            recv_sem=gather_sems.at[1, sender],
            device_id={"tm": peer},
            device_id_type=MESH,
        )

    bit, pair, pairs = lax.rem(me, 2), me // 2, n // 2
    partner = me + 1 - 2 * bit

    def relay_copy(share):
        return pltpu.make_async_remote_copy(
            src_ref=gathered.at[share],
            dst_ref=gathered.at[share],
            send_sem=relay_sems.at[share],
            recv_sem=gather_sems.at[1, share],
            device_id={"tm": partner},
            device_id_type=MESH,
        )

    def share_copy(share):
        return pltpu.make_async_copy(gathered.at[share], packed_out.at[share], share_sems.at[share])

    def over_pairs(do, way=1):
        def step(t, carry):
            do(lax.rem(pair + (1 + t if way == 1 else pairs - 1 - t), pairs))
            return carry

        lax.fori_loop(0, pairs - 1, step, 0)

    def over_peers(do):
        def step(t, carry):
            do(lax.rem(me + 1 + t, n))
            return carry

        lax.fori_loop(0, n - 1, step, 0)

    over_peers(lambda peer: energy_copy(peer, me).start())

    def rows_of(ref, share):
        return [ref[pl.ds(a * FOLD_ROWS + share * s, s)] for a in range(SIDE // FOLD_ROWS)]

    def share_of(share):
        held = SIDE // FOLD_ROWS * s * SIDE
        feet = jnp.concatenate(rows_of(foot, share), axis=0).reshape(held, comps)
        prod = jnp.dot(feet, trace[...], preferred_element_type=F32)
        back = jnp.concatenate(rows_of(backs, share), axis=0).reshape(held, frames)
        seen = jnp.concatenate(rows_of(movie, share), axis=0).reshape(held, frames)
        ferr = (prod + back.astype(F32) - seen.astype(F32)).astype(BF16)
        grad = lax.dot_general(
            ferr, trace[...], (((1,), (1,)), ((), ())), preferred_element_type=F32
        )
        grad = jnp.where(feet.astype(F32) > 0.0, grad, 0.0)
        return fold(grad.reshape(held // SIDE, SIDE, comps), s)

    def send_share(share):
        part[share] = share_of(share).astype(BF16)
        part_copy(share, me).start()

    over_peers(send_share)
    trace_copy.start()

    own[...] = share_of(me)
    energy_in[me] = energy_out[...]

    def take(peer):
        energy_copy(me, peer).wait_recv()
        part_copy(me, peer).wait_recv()
        own[...] += arrived[peer].astype(F32)
        energy_in[me] += energy_in[peer]

    over_peers(take)
    den_c = energy_in[me][:1] + RIDGE_TERM
    feet = fold(jnp.concatenate(rows_of(foot, me), axis=0).astype(F32), s)
    gathered[me] = jnp.maximum(feet - own[...] / den_c, 0.0).astype(BF16)
    gather_copy(partner, me).start()
    over_pairs(lambda other: gather_copy(2 * other + bit, me).start())
    share_copy(me).start()

    def relay(other):
        share = 2 * other + bit
        gather_copy(me, share).wait_recv()
        relay_copy(share).start()
        share_copy(share).start()

    def receive(share):
        gather_copy(me, share).wait_recv()
        share_copy(share).start()

    over_pairs(relay, -1)
    receive(partner)
    over_pairs(lambda other: receive(2 * other + 1 - bit), -1)

    for sweep in range(PASSES):
        halo_copy(sweep).wait_send()
    foot_copy.wait()
    trace_copy.wait()

    def drain(peer):
        energy_copy(peer, me).wait_send()
        part_copy(peer, me).wait_send()
        share_copy(peer).wait()

    def drain_pair(other):
        gather_copy(2 * other + bit, me).wait_send()
        relay_copy(2 * other + bit).wait_send()

    over_peers(drain)
    over_pairs(drain_pair)
    gather_copy(partner, me).wait_send()
    share_copy(me).wait()


def spread(packed, foot, trace, new_foot, new_trace):
    values = packed[...].astype(F32)
    values = jnp.where(pl.program_id(0) % 2 == 1, swap_halves(values), values)
    values = jnp.concatenate([values, values], axis=1)
    new_foot[...] = jnp.where(foot[...].astype(F32) > 0.0, values, 0.0).astype(BF16)
    new_trace[...] = trace[...]


def shards(movie, cycle_weights, footprints, traces, centre_row, centre_col, radius, comp_count):
    n = lax.axis_size("tm")
    frames = movie.shape[2]
    comps = footprints.shape[2]
    assert n % 2 == 0 and FOLD_ROWS % n == 0
    s = FOLD_ROWS // n
    blocks = SIDE // BLOCK
    tables = jnp.asarray(spread_tables(), BF16)
    vmem = pl.BlockSpec(memory_space=pltpu.VMEM)
    smem = pl.BlockSpec(memory_space=pltpu.SMEM)
    hbm = pl.BlockSpec(memory_space=pl.ANY)
    foot, trace, packed = pl.pallas_call(
        functools.partial(kernel, n, s),
        out_shape=(
            jax.ShapeDtypeStruct((SIDE, SIDE, comps), BF16),
            jax.ShapeDtypeStruct((comps, frames), BF16),
            jax.ShapeDtypeStruct((n, s * FOLD, comps), BF16),
        ),
        in_specs=[vmem] * 7 + [smem, vmem],
        out_specs=(hbm, hbm, hbm),
        scratch_shapes=[
            pltpu.VMEM((SIDE * CYCLE, comps), BF16),
            pltpu.VMEM((SIDE * CYCLE, frames), BF16),
            pltpu.VMEM((SIDE, SIDE, cycle_weights.shape[2]), BF16),
            pltpu.VMEM((SIDE, SIDE, comps), BF16),
            pltpu.VMEM((blocks, BLOCK * SIDE, SPAN * WIDE), BF16),
            pltpu.VMEM((SIDE, SIDE, frames), F32),
            pltpu.VMEM((SIDE, WIDE, frames), BF16),
            pltpu.VMEM((SIDE, SIDE, frames), BF16),
            pltpu.VMEM((SIDE, SIDE, frames), BF16),
            pltpu.VMEM((comps, frames), BF16),
            pltpu.VMEM((comps, frames), F32),
            pltpu.VMEM((comps, LANES), F32),
            pltpu.VMEM((SIDE, comps), jnp.int32),
            pltpu.VMEM((PASSES, SIDE * CYCLE, frames), BF16),
            pltpu.VMEM((PASSES, SIDE * CYCLE, frames), BF16),
            pltpu.VMEM((n, s * FOLD, comps), BF16),
            pltpu.VMEM((s * FOLD, comps), F32),
            pltpu.VMEM((n, s * FOLD, comps), BF16),
            pltpu.VMEM((8, comps), F32),
            pltpu.VMEM((n, 8, comps), F32),
            pltpu.VMEM((n, s * FOLD, comps), BF16),
            pltpu.SemaphoreType.DMA((2, PASSES)),
            pltpu.SemaphoreType.DMA((2, n)),
            pltpu.SemaphoreType.DMA((2, n)),
            pltpu.SemaphoreType.DMA((2, n)),
            pltpu.SemaphoreType.DMA((n,)),
            pltpu.SemaphoreType.DMA((2,)),
            pltpu.SemaphoreType.DMA((n,)),
        ],
        compiler_params=pltpu.CompilerParams(
            collective_id=0, has_side_effects=True, vmem_limit_bytes=60 * 1024 * 1024
        ),
    )(
        movie.reshape(SIDE, SIDE, frames),
        jnp.transpose(cycle_weights[0]),
        footprints.reshape(SIDE, SIDE, comps),
        traces.reshape(comps, frames),
        centre_row,
        centre_col,
        radius,
        comp_count,
        tables,
    )
    steps = SIDE // FOLD_ROWS
    rows = pl.BlockSpec((FOLD_ROWS, SIDE, comps), lambda a: (a, 0, 0))
    parts = pl.BlockSpec((comps // steps, frames), lambda a: (a, 0))
    new_foot, new_trace = pl.pallas_call(
        spread,
        grid=(steps,),
        out_shape=(
            jax.ShapeDtypeStruct((SIDE, SIDE, comps), BF16),
            jax.ShapeDtypeStruct((comps, frames), BF16),
        ),
        in_specs=[pl.BlockSpec((FOLD_ROWS, FOLD, comps), lambda a: (0, 0, 0)), rows, parts],
        out_specs=(rows, parts),
        compiler_params=pltpu.CompilerParams(vmem_limit_bytes=60 * 1024 * 1024),
    )(packed.reshape(FOLD_ROWS, FOLD, comps), foot, trace)
    return (new_foot.reshape(1, SIDE * SIDE, comps), new_trace[None])


def solution(mesh):
    in_specs = (
        P(("groups", "tile"), None, "tm"),
        P(("groups", "tile"), None, None),
        P(("groups", "tile"), None, None),
        P(("groups", "tile"), None, "tm"),
        P(("groups", "tile"), None),
        P(("groups", "tile"), None),
        P(("groups", "tile"), None),
        P(("groups", "tile")),
    )
    out_specs = (P(("groups", "tile"), None, None), P(("groups", "tile"), None, "tm"))
    return jax.shard_map(shards, mesh=mesh, in_specs=in_specs, out_specs=out_specs, check_vma=False)
```

```python
import functools

import jax
import jax.numpy as jnp
import numpy as np
from jax import lax
from jax.experimental import pallas as pl
from jax.experimental.pallas import tpu as pltpu
from jax.sharding import PartitionSpec as P

SIDE = 48
CYCLE = 8
WIDE = SIDE + 2 * CYCLE
FOLD_ROWS = 16
FOLD = 24
HALF = FOLD // 2
PASSES = 2
RIDGE_TERM = 1.0
BLOCK = 8
DEPTH = 16
SPAN = BLOCK + 2 * CYCLE
LANES = 128
F32 = jnp.float32
BF16 = jnp.bfloat16
MESH = pl.DeviceIdType.MESH


def cycle_offsets():
    found = []
    for row_step in range(-CYCLE, CYCLE + 1):
        for col_step in range(-CYCLE, CYCLE + 1):
            dist_sq = row_step * row_step + col_step * col_step
            if CYCLE * CYCLE <= dist_sq < (CYCLE + 1) * (CYCLE + 1):
                found.append((row_step, col_step))
    return found


def spread_tables():
    offsets = cycle_offsets()
    width = WIDE * (2 * CYCLE + 2)
    tables = np.zeros((2, len(offsets), width), np.float32)
    for index, (row_step, col_step) in enumerate(offsets):
        for odd in range(2):
            tables[odd, index, (row_step + CYCLE + odd) * WIDE + col_step + CYCLE] = 1.0
    return tables


def swap_halves(rows):
    return jnp.concatenate([rows[:, HALF:], rows[:, :HALF]], axis=1)


def fold(rows, s):
    rows = rows[:, :FOLD] + rows[:, FOLD:]
    rows = rows[:s] + swap_halves(rows[s : 2 * s]) + rows[2 * s :]
    return rows.reshape(s * FOLD, rows.shape[2])


def kernel(
    n, s, shares,
    movie, stored, prints, traces, row_at, col_at, reach, count, tables,
    new_foot, new_trace,
    feet_edge, seen_edge, weights, foot, band, pm, win, errs, backs, trace, gacc, inv_den, col_sq,
    halo_out, halo_in, part, own, arrived, energy_out, energy_in, gathered,
    halo_sems, part_sems, energy_sems, gather_sems,
):
    me = lax.axis_index("tm")
    tile = lax.axis_index("tile")
    frames = movie.shape[2]
    comps = prints.shape[2]
    blocks = SIDE // BLOCK

    barrier = pltpu.get_barrier_semaphore()
    pl.semaphore_signal(barrier, inc=1, device_id={"tile": 1 - tile}, device_id_type=MESH)

    def greet(t, carry):
        peer = lax.rem(me + 1 + t, n)
        pl.semaphore_signal(barrier, inc=1, device_id={"tm": peer}, device_id_type=MESH)
        return carry

    lax.fori_loop(0, n - 1, greet, 0)

    live_row = lax.broadcasted_iota(jnp.int32, (1, comps), 1) < count[0]
    bound = jnp.where(live_row, reach[...] * reach[...], -1)
    col_gap = lax.broadcasted_iota(jnp.int32, (SIDE, comps), 0) - col_at[...]
    col_sq[...] = col_gap * col_gap

    def mask_row(r, total):
        row_gap = r - row_at[...]
        keep = col_sq[...] <= bound - row_gap * row_gap
        kept = jnp.where(keep, prints[r].astype(F32), 0.0)
        foot[r] = kept.astype(BF16)
        return total + kept * kept

    total = lax.fori_loop(0, SIDE, mask_row, jnp.zeros((SIDE, comps), F32))
    den = jnp.sum(total, axis=0, keepdims=True) + RIDGE_TERM
    inv_den[...] = jnp.transpose(jnp.broadcast_to(1.0 / den, (LANES, comps)))
    live = lax.broadcasted_iota(jnp.int32, (comps, LANES), 0) < count[0]
    for q in range(frames // LANES):
        cols = slice(q * LANES, (q + 1) * LANES)
        trace[:, cols] = jnp.where(live, traces[:, cols].astype(F32), 0.0).astype(BF16)

    def cut_edge(j, carry):
        rows = pl.ds(j * DEPTH, DEPTH)
        spots = pl.ds(j * DEPTH * CYCLE, DEPTH * CYCLE)
        for ref, edge in ((foot, feet_edge), (movie, seen_edge)):
            whole = ref[rows].astype(F32)
            cut = jnp.where(tile == 0, whole[:, SIDE - CYCLE :], whole[:, :CYCLE])
            edge[spots] = cut.reshape(DEPTH * CYCLE, ref.shape[2]).astype(BF16)
        return carry

    lax.fori_loop(0, SIDE // DEPTH, cut_edge, 0)
    pixels = BLOCK * SIDE
    for b in range(blocks):
        turned = jnp.transpose(stored[:, b * pixels : (b + 1) * pixels].astype(F32))
        weights[b * BLOCK : (b + 1) * BLOCK] = turned.astype(BF16).reshape(BLOCK, SIDE, -1)
    pl.semaphore_wait(barrier, n)

    def halo_copy(sweep):
        return pltpu.make_async_remote_copy(
            src_ref=halo_out.at[sweep],
            dst_ref=halo_in.at[sweep],
            send_sem=halo_sems.at[0, sweep],
            recv_sem=halo_sems.at[1, sweep],
            device_id={"tile": 1 - tile},
            device_id_type=MESH,
        )

    def build_band(b, carry):
        for i in range(BLOCK):
            spread = jnp.dot(weights[b * BLOCK + i], tables[i % 2], preferred_element_type=F32)
            first = (i // 2) * LANES
            rows = slice(i * SIDE, (i + 1) * SIDE)
            if first > 0:
                band[b, rows, 0:first] = jnp.zeros((SIDE, first), BF16)
            for q in range(spread.shape[1] // LANES):
                skewed = pltpu.roll(
                    spread[:, q * LANES : (q + 1) * LANES], 0, 1, stride=1, stride_axis=0
                )
                band[b, rows, first + q * LANES : first + (q + 1) * LANES] = skewed.astype(BF16)
            last = first + spread.shape[1]
            if last < SPAN * WIDE:
                band[b, rows, last:] = jnp.zeros((SIDE, SPAN * WIDE - last), BF16)
        return carry

    for sweep in range(PASSES):

        def residual(b, carry):
            rows = pl.ds(b * DEPTH, DEPTH)
            prod = jnp.dot(
                foot[rows].reshape(DEPTH * SIDE, comps), trace[...], preferred_element_type=F32
            )
            diff = prod.reshape(DEPTH, SIDE, frames) - movie[rows].astype(F32)
            pm[rows] = diff
            return carry

        ahead = jnp.dot(feet_edge[...], trace[...], preferred_element_type=F32)
        halo_out[sweep] = (seen_edge[...].astype(F32) - ahead).astype(BF16)
        copy = halo_copy(sweep)
        copy.start()
        lax.fori_loop(0, SIDE // DEPTH, residual, 0)
        if sweep == 0:
            lax.fori_loop(0, blocks, build_band, 0)
        copy.wait_recv()

        def fill(b, carry):
            rows = pl.ds(b * BLOCK, BLOCK)
            edge = halo_in[sweep, pl.ds(b * BLOCK * CYCLE, BLOCK * CYCLE)]
            edge = edge.astype(F32).reshape(BLOCK, CYCLE, frames)
            low = jnp.where(tile == 0, 0.0, edge)
            high = jnp.where(tile == 0, edge, 0.0)
            whole = jnp.concatenate([low, -pm[rows], high], axis=1)
            win[rows] = whole.astype(BF16)
            return carry

        lax.fori_loop(0, blocks, fill, 0)

        for b in range(blocks):
            rows = slice(b * BLOCK, (b + 1) * BLOCK)
            first = b * BLOCK - CYCLE
            low, high = max(first, 0), min(first + SPAN, SIDE)
            seen = win[low:high].reshape((high - low) * WIDE, frames)
            taps = band[b, :, (low - first) * WIDE : (high - first) * WIDE]
            back = jnp.dot(taps, seen, preferred_element_type=F32).astype(BF16)
            back = back.reshape(BLOCK, SIDE, frames)
            if sweep == PASSES - 1:
                backs[rows] = back
            errs[rows] = (pm[rows] + back.astype(F32)).astype(BF16)

        gacc[...] = jnp.zeros_like(gacc)

        def descend(j, carry):
            rows = pl.ds(j * DEPTH, DEPTH)
            gacc[...] += lax.dot_general(
                foot[rows].reshape(DEPTH * SIDE, comps),
                errs[rows].reshape(DEPTH * SIDE, frames),
                (((0,), (0,)), ((), ())),
                preferred_element_type=F32,
            )
            return carry

        lax.fori_loop(0, SIDE // DEPTH, descend, 0)
        for q in range(frames // LANES):
            cols = slice(q * LANES, (q + 1) * LANES)
            moved = jnp.maximum(trace[:, cols].astype(F32) - gacc[:, cols] * inv_den[...], 0.0)
            trace[:, cols] = jnp.where(live, moved, 0.0).astype(BF16)

    new_trace[...] = trace[...]
    squares = jnp.zeros((comps, LANES), F32)
    for q in range(frames // LANES):
        now = trace[:, q * LANES : (q + 1) * LANES].astype(F32)
        squares = squares + now * now
    energy = jnp.sum(jnp.transpose(squares), axis=0, keepdims=True)
    energy_out[...] = jnp.broadcast_to(energy, energy_out.shape)

    def energy_copy(peer, sender):
        return pltpu.make_async_remote_copy(
            src_ref=energy_out,
            dst_ref=energy_in.at[sender],
            send_sem=energy_sems.at[0, peer],
            recv_sem=energy_sems.at[1, sender],
            device_id={"tm": peer},
            device_id_type=MESH,
        )

    def part_copy(peer, sender):
        return pltpu.make_async_remote_copy(
            src_ref=part.at[peer],
            dst_ref=arrived.at[sender],
            send_sem=part_sems.at[0, peer],
            recv_sem=part_sems.at[1, sender],
            device_id={"tm": peer},
            device_id_type=MESH,
        )

    def gather_copy(peer, sender):
        return pltpu.make_async_remote_copy(
            src_ref=gathered.at[sender],
            dst_ref=gathered.at[sender],
            send_sem=gather_sems.at[0, peer],
            recv_sem=gather_sems.at[1, sender],
            device_id={"tm": peer},
            device_id_type=MESH,
        )

    def owns(index, do):
        if shares == n:
            do()
        else:
            pl.when(index < shares)(do)

    def over_peers(do):
        def step(t, carry):
            do(lax.rem(me + 1 + t, n))
            return carry

        lax.fori_loop(0, n - 1, step, 0)

    over_peers(lambda peer: owns(peer, lambda: energy_copy(peer, me).start()))

    def rows_of(ref, share):
        return [ref[pl.ds(a * FOLD_ROWS + share * s, s)] for a in range(SIDE // FOLD_ROWS)]

    def share_of(share):
        held = SIDE // FOLD_ROWS * s * SIDE
        feet = jnp.concatenate(rows_of(foot, share), axis=0).reshape(held, comps)
        prod = jnp.dot(feet, trace[...], preferred_element_type=F32)
        back = jnp.concatenate(rows_of(backs, share), axis=0).reshape(held, frames)
        seen = jnp.concatenate(rows_of(movie, share), axis=0).reshape(held, frames)
        ferr = (prod + back.astype(F32) - seen.astype(F32)).astype(BF16)
        grad = lax.dot_general(
            ferr, trace[...], (((1,), (1,)), ((), ())), preferred_element_type=F32
        )
        grad = jnp.where(feet.astype(F32) > 0.0, grad, 0.0)
        return fold(grad.reshape(held // SIDE, SIDE, comps), s)

    def send_share(share):
        part[share] = share_of(share).astype(BF16)
        part_copy(share, me).start()

    over_peers(lambda peer: owns(peer, lambda: send_share(peer)))

    def settle():
        own[...] = share_of(me)
        energy_in[me] = energy_out[...]

        def take(peer):
            energy_copy(me, peer).wait_recv()
            part_copy(me, peer).wait_recv()
            own[...] += arrived[peer].astype(F32)
            energy_in[me] += energy_in[peer]

        over_peers(take)
        den_c = energy_in[me][:1] + RIDGE_TERM
        feet = fold(jnp.concatenate(rows_of(foot, me), axis=0).astype(F32), s)
        gathered[me] = jnp.maximum(feet - own[...] / den_c, 0.0).astype(BF16)
        over_peers(lambda peer: gather_copy(peer, me).start())

    owns(me, settle)

    def unfold(share):
        values = gathered[share].astype(F32).reshape(s, FOLD, comps)
        turned = swap_halves(values)
        values = jnp.concatenate([values, values], axis=1)
        turned = jnp.concatenate([turned, turned], axis=1)
        for a in range(SIDE // FOLD_ROWS):
            rows = pl.ds(a * FOLD_ROWS + share * s, s)
            new_foot[rows] = jnp.where(foot[rows].astype(F32) > 0.0, (values, turned)[a % 2], 0.0).astype(BF16)

    owns(me, lambda: unfold(me))

    def receive(peer):
        gather_copy(me, peer).wait_recv()
        unfold(peer)

    over_peers(lambda peer: owns(peer, lambda: receive(peer)))

    for sweep in range(PASSES):
        halo_copy(sweep).wait_send()

    def drain(peer):
        owns(peer, lambda: energy_copy(peer, me).wait_send())
        owns(peer, lambda: part_copy(peer, me).wait_send())
        owns(me, lambda: gather_copy(peer, me).wait_send())

    over_peers(drain)


def shards(movie, cycle_weights, footprints, traces, centre_row, centre_col, radius, comp_count):
    n = lax.axis_size("tm")
    frames = movie.shape[2]
    comps = footprints.shape[2]
    s = -(-FOLD_ROWS // n)
    while FOLD_ROWS % s:
        s += 1
    shares = FOLD_ROWS // s
    blocks = SIDE // BLOCK
    tables = jnp.asarray(spread_tables(), BF16)
    vmem = pl.BlockSpec(memory_space=pltpu.VMEM)
    smem = pl.BlockSpec(memory_space=pltpu.SMEM)
    new_foot, new_trace = pl.pallas_call(
        functools.partial(kernel, n, s, shares),
        out_shape=(
            jax.ShapeDtypeStruct((SIDE, SIDE, comps), BF16),
            jax.ShapeDtypeStruct((comps, frames), BF16),
        ),
        in_specs=[vmem] * 7 + [smem, vmem],
        out_specs=(vmem, vmem),
        scratch_shapes=[
            pltpu.VMEM((SIDE * CYCLE, comps), BF16),
            pltpu.VMEM((SIDE * CYCLE, frames), BF16),
            pltpu.VMEM((SIDE, SIDE, cycle_weights.shape[2]), BF16),
            pltpu.VMEM((SIDE, SIDE, comps), BF16),
            pltpu.VMEM((blocks, BLOCK * SIDE, SPAN * WIDE), BF16),
            pltpu.VMEM((SIDE, SIDE, frames), F32),
            pltpu.VMEM((SIDE, WIDE, frames), BF16),
            pltpu.VMEM((SIDE, SIDE, frames), BF16),
            pltpu.VMEM((SIDE, SIDE, frames), BF16),
            pltpu.VMEM((comps, frames), BF16),
            pltpu.VMEM((comps, frames), F32),
            pltpu.VMEM((comps, LANES), F32),
            pltpu.VMEM((SIDE, comps), jnp.int32),
            pltpu.VMEM((PASSES, SIDE * CYCLE, frames), BF16),
            pltpu.VMEM((PASSES, SIDE * CYCLE, frames), BF16),
            pltpu.VMEM((n, s * FOLD, comps), BF16),
            pltpu.VMEM((s * FOLD, comps), F32),
            pltpu.VMEM((n, s * FOLD, comps), BF16),
            pltpu.VMEM((8, comps), F32),
            pltpu.VMEM((n, 8, comps), F32),
            pltpu.VMEM((n, s * FOLD, comps), BF16),
            pltpu.SemaphoreType.DMA((2, PASSES)),
            pltpu.SemaphoreType.DMA((2, n)),
            pltpu.SemaphoreType.DMA((2, n)),
            pltpu.SemaphoreType.DMA((2, n)),
        ],
        compiler_params=pltpu.CompilerParams(
            collective_id=0, has_side_effects=True, vmem_limit_bytes=60 * 1024 * 1024
        ),
    )(
        movie.reshape(SIDE, SIDE, frames),
        jnp.transpose(cycle_weights[0]),
        footprints.reshape(SIDE, SIDE, comps),
        traces.reshape(comps, frames),
        centre_row,
        centre_col,
        radius,
        comp_count,
        tables,
    )
    return (new_foot.reshape(1, SIDE * SIDE, comps), new_trace[None])


def solution(mesh):
    in_specs = (
        P(("groups", "tile"), None, "tm"),
        P(("groups", "tile"), None, None),
        P(("groups", "tile"), None, None),
        P(("groups", "tile"), None, "tm"),
        P(("groups", "tile"), None),
        P(("groups", "tile"), None),
        P(("groups", "tile"), None),
        P(("groups", "tile")),
    )
    out_specs = (P(("groups", "tile"), None, None), P(("groups", "tile"), None, "tm"))
    return jax.shard_map(shards, mesh=mesh, in_specs=in_specs, out_specs=out_specs, check_vma=False)
```
